32 devices in a mesh: dp: 2 (over core), vocab: 16 (over z, y, x).
Axes of the slice: x: 2, y: 2, z: 4, core: 2. Of those that a mesh axis runs over, the one named last changes fastest.
Arguments:
- table: bfloat16 [16384, 4096], P('vocab'), may hold values from -0.75 to 0.75
- hidden: bfloat16 [512, 4096], P(('dp', 'vocab')), may hold values from -9 to 9
- cotangent: bfloat16 [512, 4096], P(('dp', 'vocab')), may hold values from -0.75 to 0.75
- input_ids: int32 [512], P('dp'), may hold values from 0 to 16383, as said below
- target_ids: int32 [512], P('dp'), may hold values from 0 to 16383
Outputs:
- table_grad: float32 [16384, 4096], P(('vocab', 'dp'))
- hidden_grad: bfloat16 [512, 4096], P(('dp', 'vocab'))
- token_loss: float32 [512], P('dp')
The draws below stay inside these ranges and needn't reach their ends.
Inputs may be any that keep to these rules, and one draw needn't show every extreme that they name: `input_ids`: the ids of one replica group may all lie in the 1024 rows of one index of vocab; in every draw some group's ids do.
All inputs are finite; a program needn't handle non-finite values.
Results may differ from the reference program's by a relative error of at most 0.0034.
Values may be sent and summed in bfloat16 or wider, within the bound.
A program may use at most 128 MiB of HBM per device.

```python
import jax
import jax.numpy as jnp
from jax import lax

D = 4096
V_DEV = 1024
MICRO = 8
MB_ROWS = 32
GROUP = 256
V = 16384
TOKENS = 512
N_DP = 2


def table_values(key):
    base = jax.random.normal(jax.random.fold_in(key, 11), (V, D), jnp.float32) * 0.125
    return jnp.clip(base, -0.75, 0.75)


def draw_table(key, part):
    return table_values(key).astype(jnp.bfloat16)


def draw_hidden(key, part):
    scales = jnp.exp(jax.random.uniform(jax.random.fold_in(key, 13), (TOKENS, 1), jnp.float32, jnp.log(0.12), jnp.log(0.5)))
    base = jax.random.normal(jax.random.fold_in(key, 12), (TOKENS, D), jnp.float32)
    return jnp.clip(base * scales, -8.0, 8.0).astype(jnp.bfloat16)


def draw_input_ids(key, part):
    groups = TOKENS // GROUP
    shards = V // V_DEV
    hot_group = jax.random.randint(jax.random.fold_in(key, 21), (), 0, groups)
    hot_shard = jax.random.randint(jax.random.fold_in(key, 22), (groups, 1), 0, shards)
    levels = jax.random.randint(jax.random.fold_in(key, 23), (groups, 1), 0, 5)
    group_index = jnp.arange(groups, dtype=jnp.int32)[:, None]
    levels = jnp.where(group_index == hot_group, 4, levels)
    pickers = jax.random.randint(jax.random.fold_in(key, 24), (groups, GROUP), 0, 4)
    concentrated = pickers < levels
    in_shard = hot_shard * V_DEV + jax.random.randint(jax.random.fold_in(key, 25), (groups, GROUP), 0, V_DEV)
    anywhere = jax.random.randint(jax.random.fold_in(key, 26), (groups, GROUP), 0, V)
    values = jnp.where(concentrated, in_shard, anywhere)
    return values.reshape(TOKENS).astype(jnp.int32)


def plant(values, stream_key, smallest, largest):
    shape = values.shape
    index_at = [jax.random.randint(jax.random.fold_in(stream_key, axis), (), 0, shape[axis]) for axis in range(len(shape))]
    values = values.at[tuple(index_at)].set(smallest)
    longest = shape.index(max(shape))
    index_at[longest] = (index_at[longest] + 1) % shape[longest]
    return values.at[tuple(index_at)].set(largest)


def shard_levels(own_key, dims, split, smallest, largest):
    def one(axis_at, parts):
        heights = jax.random.uniform(jax.random.fold_in(jax.random.fold_in(own_key, 6), axis_at), (parts,), jnp.float32, smallest / len(split), largest / len(split))
        return jnp.repeat(jnp.exp(heights), dims[axis_at] // parts).reshape((-1,) + (1,) * (len(dims) - axis_at - 1))

    loudness = one(*split[0])
    for cut in split[1:]:
        loudness = loudness * one(*cut)
    return loudness


def centred(stream_key, extent, deviation, reach, cuts=(), kind=jnp.bfloat16):
    values = jax.random.normal(stream_key, extent, jnp.float32) * deviation
    if len(cuts) > 0:
        values = shard_levels(stream_key, extent, cuts, -0.22, 0.18) * values
    return jnp.clip(values, min=-reach, max=reach).astype(kind)


def setup_inputs(seed: int = 0) -> dict:
    keys = jax.random.split(jax.random.key(seed), 6)
    return {
        "table": draw_table(jax.random.fold_in(keys[5], 71), 0),
        "hidden": draw_hidden(jax.random.fold_in(keys[5], 71), 0),
        "cotangent": centred(keys[2], (TOKENS, D), 0.05, 0.75, ((0, 32),)),
        "input_ids": draw_input_ids(jax.random.fold_in(keys[5], 71), 0),
        "target_ids": plant(jax.random.randint(keys[4], (TOKENS,), 0, V), jax.random.fold_in(keys[4], 1), 0, V - 1).astype(jnp.int32),
    }


def reference(table, hidden, cotangent, input_ids, target_ids):
    group = MICRO * MB_ROWS
    vocab_rows = table.shape[0]
    width = table.shape[1]
    columns = jnp.arange(vocab_rows, dtype=jnp.int32)

    def one_group(total, index):
        begin = (index * group).astype(jnp.int32)
        rows = lax.dynamic_slice_in_dim(hidden, begin, group, 0)
        incoming = lax.dynamic_slice_in_dim(cotangent, begin, group, 0)
        inputs = lax.dynamic_slice_in_dim(input_ids, begin, group, 0)
        targets = lax.dynamic_slice_in_dim(target_ids, begin, group, 0)
        logits = lax.dot_general(rows, table, (((1,), (1,)), ((), ())), preferred_element_type=jnp.float32)
        top = jnp.max(logits, axis=1)
        lse = top + jnp.log(jnp.sum(jnp.exp(logits - top[:, None]), axis=1))
        hit = targets[:, None] == columns[None, :]
        picked = jnp.sum(jnp.where(hit, logits, jnp.float32(0.0)), axis=1)
        loss = lse - picked
        probs = jnp.exp(logits - lse[:, None])
        dlogits = (probs - hit.astype(jnp.float32)).astype(jnp.bfloat16)
        row_grad = jnp.dot(dlogits, table, preferred_element_type=jnp.float32).astype(jnp.bfloat16)
        grad = lax.dot_general(dlogits, rows, (((0,), (0,)), ((), ())), preferred_element_type=jnp.float32)
        grad = grad.at[inputs].add(incoming.astype(jnp.float32))
        return total + grad, (row_grad, loss)

    start = jnp.zeros((vocab_rows, width), jnp.float32)
    total, (row_grads, losses) = lax.scan(one_group, start, jnp.arange(N_DP, dtype=jnp.int32))
    return total, row_grads.reshape(-1, width), losses.reshape(-1)
```

```python
import functools

import jax
import jax.numpy as jnp
from jax import lax
from jax.experimental import pallas as pl
from jax.experimental.pallas import tpu as pltpu
from jax.sharding import PartitionSpec as P

MESH = pl.DeviceIdType.MESH
BF16 = jnp.bfloat16
F32 = jnp.float32
WIRE1 = BF16
WIRE2 = BF16
WIREZ = BF16


def kernel(groups, n, table_hbm, hidden_ref, cot_ref, in_ids_ref, tgt_ids_ref,
           x_all, e_all, hg_ref, loss_ref,
           table, x_own, logits, st, own_e, part, s1, r1, s2, r2, s3, r3,
           load_sem, local_sem, send, recv):
    nz = n // 4
    rows, width = hidden_ref.shape
    shard = table.shape[0]
    tokens = n * rows
    piece = shard // groups
    half = width // 2
    me = lax.axis_index("vocab")
    g = lax.axis_index("dp")
    z = me // 4
    y = (me % 4) // 2
    x = me % 2
    slots = iter(range(send.shape[0]))

    def at(zz, yy, xx):
        return zz * 4 + yy * 2 + xx

    x_peer = at(z, y, 1 - x)
    y_peer = at(z, 1 - y, x)

    load = pltpu.make_async_copy(table_hbm, table, load_sem)
    load.start()

    barrier = pltpu.get_barrier_semaphore()
    for d in range(1, n):
        pl.semaphore_signal(barrier, inc=1, device_id=(g, (me + d) % n), device_id_type=MESH)
    for d in range(1, groups):
        pl.semaphore_signal(barrier, inc=1, device_id=((g + d) % groups, me), device_id_type=MESH)
    pl.semaphore_wait(barrier, n - 1 + groups - 1)

    started = []

    def push(src, dst, v, gg=None):
        k = next(slots)
        c = pltpu.make_async_remote_copy(
            src_ref=src, dst_ref=dst, send_sem=send.at[k], recv_sem=recv.at[k],
            device_id=(g if gg is None else gg, v), device_id_type=MESH)
        c.start()
        started.append(c)
        return c

    left = pl.ds(0, half)
    right = pl.ds(half, half)

    def gather_first(kind, own):
        dst = x_own.at[kind, me]
        fx = [push(own, dst, x_peer)]
        fy = [push(own, dst, y_peer)]
        fz = [push(own, dst, at((z + d) % nz, y, x)) for d in range(1, nz)]
        return fx, fy, fz

    def gather_second(kind, state):
        fx, fy, fz = state
        for d in range(1, nz):
            fz[d - 1].wait_recv()
            blk = x_own.at[kind, at((z + nz - d) % nz, y, x)]
            fx.append(push(blk, blk, x_peer))
            fy.append(push(blk, blk, y_peer))

    def gather_third(kind, state):
        fx, fy, _ = state
        out = []
        for d in range(nz):
            zz = (z + nz - d) % nz
            fx[d].wait_recv()
            blk = x_own.at[kind, at(zz, y, 1 - x), :, left]
            out.append(push(blk, blk, y_peer))
            fy[d].wait_recv()
            blk = x_own.at[kind, at(zz, 1 - y, x), :, right]
            out.append(push(blk, blk, x_peer))
        return out

    local = []

    def spread(kind):
        c = pltpu.make_async_copy(x_own.at[kind], x_all.at[g, kind], local_sem.at[kind])
        c.start()
        local.append(c)
        return [push(x_own.at[kind], x_all.at[g, kind], me, (g + d) % groups) for d in range(1, groups)]

    state = gather_first(0, hidden_ref)
    x_own[0, pl.ds(me, 1)] = hidden_ref[...][None]
    x_own[1, pl.ds(me, 1)] = cot_ref[...][None]
    gather_second(0, state)
    tail = gather_third(0, state)
    cot_state = gather_first(1, cot_ref)
    offset = me * shard
    step = 256
    for i in range(0, shard, step):
        vocab_row = offset + i + lax.broadcasted_iota(jnp.int32, (step, tokens), 0)
        own_e[1, i:i + step] = (vocab_row == in_ids_ref[...]).astype(F32).astype(BF16)
    for c in tail:
        c.wait_recv()
    late = spread(0)
    load.wait()
    h = x_own[0].reshape(tokens, width)
    top = jnp.full((1, tokens), -jnp.inf, F32)
    for i in range(0, shard, step):
        lg = lax.dot_general(table[i:i + step], h, (((1,), (1,)), ((), ())), preferred_element_type=F32)
        logits[i:i + step] = lg
        top = jnp.maximum(top, jnp.max(lg, axis=0, keepdims=True))
    total = jnp.zeros((1, tokens), F32)
    pick = jnp.zeros((1, tokens), F32)
    tgt = tgt_ids_ref[...]
    for i in range(0, shard, step):
        lg = logits[i:i + step]
        vocab_row = offset + i + lax.broadcasted_iota(jnp.int32, (step, tokens), 0)
        total = total + jnp.sum(jnp.exp(lg - top), axis=0, keepdims=True)
        pick = pick + jnp.sum(jnp.where(vocab_row == tgt, lg, 0.0), axis=0, keepdims=True)
    line = lax.broadcasted_iota(jnp.int32, (8, tokens), 0)
    mine = jnp.where(line == 0, top, jnp.where(line == 1, total, pick))
    st[pl.ds(me, 1)] = mine[None]
    stats = [push(st.at[me], st.at[me], (me + d) % n) for d in range(1, n)]
    gather_second(1, cot_state)
    for c in stats:
        c.wait_recv()
    top = st[0, 0:1]
    for j in range(1, n):
        top = jnp.maximum(top, st[j, 0:1])
    total = jnp.zeros((1, tokens), F32)
    pick = jnp.zeros((1, tokens), F32)
    for j in range(n):
        total = total + st[j, 1:2] * jnp.exp(st[j, 0:1] - top)
        pick = pick + st[j, 2:3]
    lse = top + jnp.log(total)
    loss_ref[...] = lse - pick
    for i in range(0, shard, step):
        vocab_row = offset + i + lax.broadcasted_iota(jnp.int32, (step, tokens), 0)
        hit = (vocab_row == tgt).astype(F32)
        own_e[0, i:i + step] = (jnp.exp(logits[i:i + step] - lse) - hit).astype(BF16)

    dl = own_e[0]
    cols = 512

    def product(i):
        p = lax.dot_general(dl, table[:, i:i + cols], (((0,), (0,)), ((), ())), preferred_element_type=F32)
        part[:, :, :, :, i:i + cols] = p.reshape(nz, 2, 2, rows, cols)

    for i in range(0, half, cols):
        product(i)
    s1[0] = part[:, pl.ds(1 - y, 1), :, :, 0:half].reshape(nz, 2, rows, half).astype(WIRE1)
    ca = push(s1.at[0], r1.at[0], y_peer)
    for i in range(half, width, cols):
        product(i)
    s1[1] = part[:, :, pl.ds(1 - x, 1), :, half:width].reshape(nz, 2, rows, half).astype(WIRE1)
    cb = push(s1.at[1], r1.at[1], x_peer)

    for kind in range(2):
        dst = e_all.at[:, pl.ds(pl.multiple_of((g * 2 + kind) * tokens, tokens), tokens)]
        c = pltpu.make_async_copy(
            own_e.at[kind, pl.ds(pl.multiple_of(g * piece, piece), piece)], dst, local_sem.at[2 + kind])
        c.start()
        local.append(c)
        for d in range(1, groups):
            peer = (g + d) % groups
            late.append(push(own_e.at[kind, pl.ds(pl.multiple_of(peer * piece, piece), piece)], dst, me, peer))

    cot_tail = gather_third(1, cot_state)

    ca.wait_recv()
    s2[0] = (part[:, pl.ds(y, 1), pl.ds(1 - x, 1), :, 0:half].reshape(nz, rows, half)
             + r1[0, :, pl.ds(1 - x, 1)].reshape(nz, rows, half).astype(F32)).astype(WIRE2)
    da = push(s2.at[0], r2.at[0], x_peer)
    cb.wait_recv()
    s2[1] = (part[:, pl.ds(1 - y, 1), pl.ds(x, 1), :, half:width].reshape(nz, rows, half)
             + r1[1, :, pl.ds(1 - y, 1)].reshape(nz, rows, half).astype(F32)).astype(WIRE2)
    db = push(s2.at[1], r2.at[1], y_peer)

    def merged(side, zz):
        a = part[pl.ds(zz, 1), pl.ds(y, 1), pl.ds(x, 1), :, side * half:(side + 1) * half].reshape(rows, half)
        b = r1[side, pl.ds(zz, 1), pl.ds(x if side == 0 else y, 1)].reshape(rows, half).astype(F32)
        return a + b + r2[side, pl.ds(zz, 1)].reshape(rows, half).astype(F32)

    last = []
    for side, c in ((0, da), (1, db)):
        c.wait_recv()
        for d in range(1, nz):
            zz = (z + d) % nz
            s3[side, d - 1] = merged(side, zz).astype(WIREZ)
            last.append(push(s3.at[side, d - 1], r3.at[side, d - 1], at(zz, y, x)))
    for c in cot_tail:
        c.wait_recv()
    late += spread(1)
    for c in last:
        c.wait_recv()
    for side in range(2):
        acc = merged(side, z)
        for d in range(1, nz):
            acc = acc + r3[side, d - 1].astype(F32)
        hg_ref[:, side * half:(side + 1) * half] = acc.astype(BF16)
    for c in late:
        c.wait_recv()
    for c in local:
        c.wait()
    for c in started:
        c.wait_send()


def solution(mesh):
    groups, n = mesh.shape["dp"], mesh.shape["vocab"]

    def body(table, hidden, cotangent, input_ids, target_ids):
        rows, width = hidden.shape
        shard = table.shape[0]
        nz = n // 4
        tokens = n * rows
        half = width // 2
        piece = shard // groups
        copies = 2 * (nz + 1 + 2 * (nz - 1) + 2 * nz) + 2 * (groups - 1) + (n - 1) + 2 + 2 * (groups - 1) + 2 + 2 * (nz - 1)
        vmem = pl.BlockSpec(memory_space=pltpu.VMEM)
        anys = pl.BlockSpec(memory_space=pl.ANY)
        x_all, e_all, hg, loss = pl.pallas_call(
            functools.partial(kernel, groups, n),
            out_shape=(
                jax.ShapeDtypeStruct((groups, 2, n, rows, width), BF16),
                jax.ShapeDtypeStruct((piece, groups * 2 * tokens), BF16),
                jax.ShapeDtypeStruct((rows, width), BF16),
                jax.ShapeDtypeStruct((1, tokens), F32),
            ),
            in_specs=[anys, vmem, vmem, vmem, vmem],
            out_specs=(anys, anys, vmem, vmem),
            scratch_shapes=[
                pltpu.VMEM((shard, width), BF16),
                pltpu.VMEM((2, n, rows, width), BF16),
                pltpu.VMEM((shard, tokens), F32),
                pltpu.VMEM((n, 8, tokens), F32),
                pltpu.VMEM((2, shard, tokens), BF16),
                pltpu.VMEM((nz, 2, 2, rows, width), F32),
                pltpu.VMEM((2, nz, 2, rows, half), WIRE1),
                pltpu.VMEM((2, nz, 2, rows, half), WIRE1),
                pltpu.VMEM((2, nz, rows, half), WIRE2),
                pltpu.VMEM((2, nz, rows, half), WIRE2),
                pltpu.VMEM((2, nz - 1, rows, half), WIREZ),
                pltpu.VMEM((2, nz - 1, rows, half), WIREZ),
                pltpu.SemaphoreType.DMA,
                pltpu.SemaphoreType.DMA((4,)),
                pltpu.SemaphoreType.DMA((copies,)),
                pltpu.SemaphoreType.DMA((copies,)),
            ],
            compiler_params=pltpu.CompilerParams(
                collective_id=0, has_side_effects=True, vmem_limit_bytes=56 * 2**20),
        )(table, hidden, cotangent, input_ids.reshape(1, tokens), target_ids.reshape(1, tokens))
        table_grad = jnp.dot(
            e_all, x_all.reshape(groups * 2 * tokens, width), preferred_element_type=F32)
        return table_grad, hg, loss.reshape(tokens)

    return jax.shard_map(
        body,
        mesh=mesh,
        in_specs=(
            P("vocab", None),
            P(("dp", "vocab"), None),
            P(("dp", "vocab"), None),
            P("dp"),
            P("dp"),
        ),
        out_specs=(P(("vocab", "dp"), None), P(("dp", "vocab"), None), P("dp")),
        check_vma=False,
    )
```

```python
import functools

import jax
import jax.numpy as jnp
from jax import lax
from jax.experimental import pallas as pl
from jax.experimental.pallas import tpu as pltpu
from jax.sharding import PartitionSpec as P

MESH = pl.DeviceIdType.MESH
BF16 = jnp.bfloat16
F32 = jnp.float32
WIRE1 = BF16
WIRE2 = BF16
WIREZ = BF16
CHUNKS = 2


def kernel(groups, n, table_hbm, hidden_ref, cot_ref, in_ids_ref, tgt_ids_ref,
           x_all, e_all, hg_ref, loss_ref,
           table, x_own, logits, st, own_e, part, s1, r1, s2, r2, s3, r3,
           load_sem, local_sem, send, recv):
    nz = n // 4
    rows, width = hidden_ref.shape
    shard = table.shape[0]
    tokens = n * rows
    piece = shard // groups
    half = width // 2
    me = lax.axis_index("vocab")
    g = lax.axis_index("dp")
    z = me // 4
    y = (me % 4) // 2
    x = me % 2
    slots = iter(range(send.shape[0]))

    def at(zz, yy, xx):
        return zz * 4 + yy * 2 + xx

    x_peer = at(z, y, 1 - x)
    y_peer = at(z, 1 - y, x)

    load = pltpu.make_async_copy(table_hbm, table, load_sem)
    load.start()

    barrier = pltpu.get_barrier_semaphore()
    for d in range(1, n):
        pl.semaphore_signal(barrier, inc=1, device_id=(g, (me + d) % n), device_id_type=MESH)
    for d in range(1, groups):
        pl.semaphore_signal(barrier, inc=1, device_id=((g + d) % groups, me), device_id_type=MESH)
    pl.semaphore_wait(barrier, n - 1 + groups - 1)

    started = []

    def when(cond, act):
        if cond is None:
            act()
        else:
            pl.when(cond)(act)

    def both(a, b):
        return b if a is None else jnp.logical_and(a, b)

    def push(src, dst, v, gg=None, cond=None):
        k = next(slots)
        c = pltpu.make_async_remote_copy(
            src_ref=src, dst_ref=dst, send_sem=send.at[k], recv_sem=recv.at[k],
            device_id=(g if gg is None else gg, v), device_id_type=MESH)
        when(cond, c.start)
        started.append((cond, c))
        return c

    above, below = z + 1 < nz, z > 0
    up, down = at(jnp.minimum(z + 1, nz - 1), y, x), at(jnp.maximum(z - 1, 0), y, x)

    def gather_first(kind, own, base, span):
        own = own.at[:, pl.ds(base, span)]
        dst = x_own.at[kind, me, :, pl.ds(base, span)]
        ups = push(own, dst, up, cond=above)
        downs = push(own, dst, down, cond=below)
        return [(None, z, push(own, dst, x_peer), push(own, dst, y_peer))], ups, downs, kind, base, span

    def gather_second(state):
        seen, ups, downs, kind, base, span = state
        for s in range(nz - 1):
            for inward, cond, zz, go, nxt in ((ups, z - 1 - s >= 0, jnp.maximum(z - 1 - s, 0), above, up),
                                              (downs, z + 1 + s < nz, jnp.minimum(z + 1 + s, nz - 1), below, down)):
                when(cond, inward.wait_recv)
                blk = x_own.at[kind, at(zz, y, x), :, pl.ds(base, span)]
                if s < nz - 2:
                    c = push(blk, blk, nxt, cond=both(cond, go))
                    if nxt is up:
                        ups = c
                    else:
                        downs = c
                seen.append((cond, zz, push(blk, blk, x_peer, cond=cond), push(blk, blk, y_peer, cond=cond)))

    def gather_third(state):
        seen, _, _, kind, base, span = state
        left = pl.ds(base, span // 2)
        right = pl.ds(base + span // 2, span // 2)
        out = []
        for cond, zz, fx, fy in seen:
            when(cond, fx.wait_recv)
            blk = x_own.at[kind, at(zz, y, 1 - x), :, left]
            out.append((cond, push(blk, blk, y_peer, cond=cond)))
            when(cond, fy.wait_recv)
            blk = x_own.at[kind, at(zz, 1 - y, x), :, right]
            out.append((cond, push(blk, blk, x_peer, cond=cond)))
        return out

    local = []

    def spread(kind):
        c = pltpu.make_async_copy(x_own.at[kind], x_all.at[g, kind], local_sem.at[kind])
        c.start()
        local.append(c)
        return [push(x_own.at[kind], x_all.at[g, kind], me, (g + d) % groups) for d in range(1, groups)]

    states = [gather_first(0, hidden_ref, i * half, half) for i in range(2)]
    x_own[0, pl.ds(me, 1)] = hidden_ref[...][None]
    x_own[1, pl.ds(me, 1)] = cot_ref[...][None]
    tails = []
    for state in states:
        gather_second(state)
        tails.append(gather_third(state))
    cot_state = gather_first(1, cot_ref, 0, width)
    offset = me * shard
    step = 256
    for i in range(0, shard, step):
        vocab_row = offset + i + lax.broadcasted_iota(jnp.int32, (step, tokens), 0)
        own_e[1, i:i + step] = (vocab_row == in_ids_ref[...]).astype(F32).astype(BF16)
    load.wait()
    top = jnp.full((1, tokens), -jnp.inf, F32)
    for k in range(2):
        for cond, c in tails[k]:
            when(cond, c.wait_recv)
        h = x_own[0, :, :, k * half:(k + 1) * half].reshape(tokens, half)
        for i in range(0, shard, step):
            lg = lax.dot_general(table[i:i + step, k * half:(k + 1) * half], h, (((1,), (1,)), ((), ())),
                                 preferred_element_type=F32)
            if k == 1:
                lg = lg + logits[i:i + step]
                top = jnp.maximum(top, jnp.max(lg, axis=0, keepdims=True))
            logits[i:i + step] = lg
    late = spread(0)
    total = jnp.zeros((1, tokens), F32)
    pick = jnp.zeros((1, tokens), F32)
    tgt = tgt_ids_ref[...]
    for i in range(0, shard, step):
        lg = logits[i:i + step]
        vocab_row = offset + i + lax.broadcasted_iota(jnp.int32, (step, tokens), 0)
        total = total + jnp.sum(jnp.exp(lg - top), axis=0, keepdims=True)
        pick = pick + jnp.sum(jnp.where(vocab_row == tgt, lg, 0.0), axis=0, keepdims=True)
    line = lax.broadcasted_iota(jnp.int32, (8, tokens), 0)
    mine = jnp.where(line == 0, top, jnp.where(line == 1, total, pick))
    st[pl.ds(me, 1)] = mine[None]
    stats = [push(st.at[me], st.at[me], (me + d) % n) for d in range(1, n)]
    gather_second(cot_state)
    for c in stats:
        c.wait_recv()
    top = st[0, 0:1]
    for j in range(1, n):
        top = jnp.maximum(top, st[j, 0:1])
    total = jnp.zeros((1, tokens), F32)
    pick = jnp.zeros((1, tokens), F32)
    for j in range(n):
        total = total + st[j, 1:2] * jnp.exp(st[j, 0:1] - top)
        pick = pick + st[j, 2:3]
    lse = top + jnp.log(total)
    loss_ref[...] = lse - pick
    for i in range(0, shard, step):
        vocab_row = offset + i + lax.broadcasted_iota(jnp.int32, (step, tokens), 0)
        hit = (vocab_row == tgt).astype(F32)
        own_e[0, i:i + step] = (jnp.exp(logits[i:i + step] - lse) - hit).astype(BF16)

    dl = own_e[0]
    cols = 512

    def product(i):
        p = lax.dot_general(dl, table[:, i:i + cols], (((0,), (0,)), ((), ())), preferred_element_type=F32)
        part[:, :, :, :, i:i + cols] = p.reshape(nz, 2, 2, rows, cols)

    wide = half // CHUNKS
    firsts = [[], []]
    for c in range(CHUNKS):
        for side in range(2):
            lo = side * half + c * wide
            for i in range(lo, lo + wide, cols):
                product(i)
            if side == 0:
                p = part[:, pl.ds(1 - y, 1), :, :, lo:lo + wide]
            else:
                p = part[:, :, pl.ds(1 - x, 1), :, lo:lo + wide]
            s1[side, c] = p.reshape(nz, 2, rows, wide).astype(WIRE1)
            firsts[side].append(push(s1.at[side, c], r1.at[side, c], y_peer if side == 0 else x_peer))

    for kind in range(2):
        dst = e_all.at[:, pl.ds(pl.multiple_of((g * 2 + kind) * tokens, tokens), tokens)]
        c = pltpu.make_async_copy(
            own_e.at[kind, pl.ds(pl.multiple_of(g * piece, piece), piece)], dst, local_sem.at[2 + kind])
        c.start()
        local.append(c)
        for d in range(1, groups):
            peer = (g + d) % groups
            late.append(push(own_e.at[kind, pl.ds(pl.multiple_of(peer * piece, piece), piece)], dst, me, peer))

    def merged_first(side, c, zz, yy, xx, count):
        lo = side * half + c * wide
        a = part[pl.ds(zz, count), pl.ds(yy, 1), pl.ds(xx, 1), :, lo:lo + wide].reshape(count, rows, wide)
        b = r1[side, c, pl.ds(zz, count), pl.ds(xx if side == 0 else yy, 1)].reshape(count, rows, wide)
        return a + b.astype(F32)

    seconds = [[], []]
    for c in range(CHUNKS):
        for side in range(2):
            firsts[side][c].wait_recv()
            yy, xx, peer = (y, 1 - x, x_peer) if side == 0 else (1 - y, x, y_peer)
            s2[side, c] = merged_first(side, c, 0, yy, xx, nz).astype(WIRE2)
            seconds[side].append(push(s2.at[side, c], r2.at[side, c], peer))

    cot_tail = gather_third(cot_state)

    def merged(side, c, zz):
        return (merged_first(side, c, zz, y, x, 1)
                + r2[side, c, pl.ds(zz, 1)].astype(F32)).reshape(rows, wide)

    last = []
    for c in range(CHUNKS):
        for side in range(2):
            seconds[side][c].wait_recv()
            for d in range(1, nz):
                zz = (z + d) % nz
                s3[side, c, d - 1] = merged(side, c, zz).astype(WIREZ)
                last.append(push(s3.at[side, c, d - 1], r3.at[side, c, d - 1], at(zz, y, x)))
    for cond, c in cot_tail:
        when(cond, c.wait_recv)
    late += spread(1)
    for c in last:
        c.wait_recv()
    for c in range(CHUNKS):
        for side in range(2):
            acc = merged(side, c, z)
            for d in range(1, nz):
                acc = acc + r3[side, c, d - 1].astype(F32)
            lo = side * half + c * wide
            hg_ref[:, lo:lo + wide] = acc.astype(BF16)
    for c in late:
        c.wait_recv()
    for c in local:
        c.wait()
    for cond, c in started:
        when(cond, c.wait_send)


def weight_kernel(e_ref, x_ref, out_ref):
    out_ref[...] = jnp.dot(e_ref[...], x_ref[...], preferred_element_type=F32)


def weight_grad(e, x):
    tile = 512
    return pl.pallas_call(
        weight_kernel,
        grid=(x.shape[1] // tile,),
        out_shape=jax.ShapeDtypeStruct((e.shape[0], x.shape[1]), F32),
        in_specs=[
            pl.BlockSpec(e.shape, lambda i: (0, 0)),
            pl.BlockSpec((x.shape[0], tile), lambda i: (0, i)),
        ],
        out_specs=pl.BlockSpec((e.shape[0], tile), lambda i: (0, i)),
        compiler_params=pltpu.CompilerParams(vmem_limit_bytes=60 * 2**20),
    )(e, x)


def solution(mesh):
    groups, n = mesh.shape["dp"], mesh.shape["vocab"]

    def body(table, hidden, cotangent, input_ids, target_ids):
        rows, width = hidden.shape
        shard = table.shape[0]
        nz = n // 4
        tokens = n * rows
        half = width // 2
        piece = shard // groups
        copies = 3 * (4 + 2 * (nz - 2) + 8 * (nz - 1) + 2) + 2 * (groups - 1) + (n - 1) + 2 * (groups - 1) + CHUNKS * (4 + 2 * (nz - 1))
        wide = half // CHUNKS
        vmem = pl.BlockSpec(memory_space=pltpu.VMEM)
        anys = pl.BlockSpec(memory_space=pl.ANY)
        x_all, e_all, hg, loss = pl.pallas_call(
            functools.partial(kernel, groups, n),
            out_shape=(
                jax.ShapeDtypeStruct((groups, 2, n, rows, width), BF16),
                jax.ShapeDtypeStruct((piece, groups * 2 * tokens), BF16),
                jax.ShapeDtypeStruct((rows, width), BF16),
                jax.ShapeDtypeStruct((1, tokens), F32),
            ),
            in_specs=[anys, vmem, vmem, vmem, vmem],
            out_specs=(anys, anys, vmem, vmem),
            scratch_shapes=[
                pltpu.VMEM((shard, width), BF16),
                pltpu.VMEM((2, n, rows, width), BF16),
                pltpu.VMEM((shard, tokens), F32),
                pltpu.VMEM((n, 8, tokens), F32),
                pltpu.VMEM((2, shard, tokens), BF16),
                pltpu.VMEM((nz, 2, 2, rows, width), F32),
                pltpu.VMEM((2, CHUNKS, nz, 2, rows, wide), WIRE1),
                pltpu.VMEM((2, CHUNKS, nz, 2, rows, wide), WIRE1),
                pltpu.VMEM((2, CHUNKS, nz, rows, wide), WIRE2),
                pltpu.VMEM((2, CHUNKS, nz, rows, wide), WIRE2),
                pltpu.VMEM((2, CHUNKS, nz - 1, rows, wide), WIREZ),
                pltpu.VMEM((2, CHUNKS, nz - 1, rows, wide), WIREZ),
                pltpu.SemaphoreType.DMA,
                pltpu.SemaphoreType.DMA((4,)),
                pltpu.SemaphoreType.DMA((copies,)),
                pltpu.SemaphoreType.DMA((copies,)),
            ],
            compiler_params=pltpu.CompilerParams(
                collective_id=0, has_side_effects=True, vmem_limit_bytes=56 * 2**20),
        )(table, hidden, cotangent, input_ids.reshape(1, tokens), target_ids.reshape(1, tokens))
        table_grad = weight_grad(e_all, x_all.reshape(groups * 2 * tokens, width))
        return table_grad, hg, loss.reshape(tokens)

    return jax.shard_map(
        body,
        mesh=mesh,
        in_specs=(
            P("vocab", None),
            P(("dp", "vocab"), None),
            P(("dp", "vocab"), None),
            P("dp"),
            P("dp"),
        ),
        out_specs=(P(("vocab", "dp"), None), P(("dp", "vocab"), None), P("dp")),
        check_vma=False,
    )
```
